32 devices in a mesh: dp: 4 (over y, x), land: 8 (over z, core).
Axes of the slice: x: 2, y: 2, z: 4, core: 2. Of those that a mesh axis runs over, the one named last changes fastest.
Arguments:
- items: bfloat16 [16384, 768], P(('dp', 'land')), may hold values from -1.5 to 1.5
- landmarks: bfloat16 [8192, 768], P('land'), may hold values from -1.5 to 1.5
- scales: float32 [8192], P('land'), may hold values from 0.25 to 1
- eigvecs: bfloat16 [8192, 256], P('land'), may hold values from -0.0625 to 0.0625
- eigvals: float32 [256], replicated, may hold values from 0.5 to 2
Outputs:
- coords: float32 [16384, 256], P(('dp', 'land'))
- gram: float32 [256, 256], replicated
The draws below stay inside these ranges and needn't reach their ends.
All inputs are finite; a program needn't handle non-finite values.
Results may differ from the reference program's by a relative error of at most 0.0028.
Values may be sent and summed in bfloat16 or wider, within the bound.
No kernel may reach another device: no remote copies, remote signals or barrier semaphores. Data moves between devices by JAX's collectives and lax.ppermute only.
A program may use at most 128 MiB of HBM per device.

```python
import math
import jax
import jax.numpy as jnp
from jax import lax

D = 768
K = 256
LAND_DEV = 1024
ROW_DEV = 512
LANDMARKS = 8192
NROWS = 16384
N_LAND = 8


latent_dims = 16


def shared_basis(key):
    basis = jax.random.normal(jax.random.fold_in(key, 7), (D, latent_dims), jnp.float32)
    basis = jnp.clip(basis, -4.0, 4.0) / jnp.sqrt(jnp.float32(D))
    return basis


def base_latent(key, count, salt):
    latent = jnp.clip(jax.random.normal(jax.random.fold_in(key, salt), (count, latent_dims), jnp.float32), -4.0, 4.0)
    noise = jnp.clip(jax.random.normal(jax.random.fold_in(key, salt + 1), (count, D), jnp.float32), -4.0, 4.0)
    return (latent, noise)


def embed_points(key, latent, noise):
    spread = jnp.sqrt(jnp.float32(3.0 / latent_dims))
    values = jnp.dot(latent * spread, shared_basis(key).T, precision=lax.Precision.HIGHEST)
    values = values + noise * jnp.sqrt(jnp.float32(0.25) / jnp.float32(D))
    return jnp.clip(values, -1.5, 1.5).astype(jnp.bfloat16)


def block_layout(key):
    block_count = NROWS // ROW_DEV
    land_count = LANDMARKS // LAND_DEV
    group_count = block_count // land_count
    block_ids = jnp.arange(block_count)
    group_pos = ((block_ids // land_count).astype(jnp.float32) + 0.5) / jnp.float32(group_count) - 0.5
    land_pos = ((block_ids % land_count).astype(jnp.float32) + 0.5) / jnp.float32(land_count) - 0.5
    signs = jnp.where(jax.random.uniform(jax.random.fold_in(key, 41), (2,), jnp.float32) < 0.5, -1.0, 1.0)
    jitter = jax.random.uniform(jax.random.fold_in(key, 43), (block_count,), jnp.float32, -0.25, 0.25)
    log_scale = 0.7 * signs[0] * group_pos + 0.4 * signs[1] * land_pos + jitter
    directions = jax.random.normal(jax.random.fold_in(key, 45), (2, latent_dims), jnp.float32)
    directions = directions / jnp.sqrt(jnp.sum(directions * directions, axis=1, keepdims=True))
    wobble = jnp.clip(jax.random.normal(jax.random.fold_in(key, 47), (block_count, latent_dims), jnp.float32), -4.0, 4.0)
    offsets = 3.0 * group_pos[:, None] * directions[0][None, :] + 2.0 * land_pos[:, None] * directions[1][None, :] + 0.25 * wobble
    return (jnp.exp(log_scale), offsets)


def draw_items(key, part):
    latent, noise = base_latent(key, NROWS, 21)
    stretch, offsets = block_layout(key)
    block_count = NROWS // ROW_DEV
    latent = latent.reshape(block_count, ROW_DEV, latent_dims) * stretch[:, None, None] + offsets[:, None, :]
    return embed_points(key, latent.reshape(NROWS, latent_dims), noise)


def draw_landmarks(key, part):
    latent, noise = base_latent(key, LANDMARKS, 31)
    return embed_points(key, latent * 1.3, noise)


def block_levels(own_key, dims, shards, low, high):
    factor_of, own = 1.0, jax.random.fold_in(own_key, 6)
    for position, blocks in shards:
        draws = jnp.exp(jax.random.uniform(jax.random.fold_in(own, position), (blocks,), jnp.float32, low / len(shards), high / len(shards)))
        factor_of = factor_of * jnp.repeat(draws, dims[position] // blocks).reshape([-1 if axis == position else 1 for axis in range(len(dims))])
    return factor_of


def normal_values(own_key, extent, scale, limit, shards=(), held_as=jnp.bfloat16):
    entries = scale * jax.random.normal(own_key, extent, jnp.float32)
    if shards:
        entries = entries * block_levels(own_key, extent, shards, -0.22, 0.18)
    return jnp.clip(entries, -limit, limit).astype(held_as)


def setup_inputs(seed: int = 0) -> dict:
    key_list = jax.random.split(jax.random.key(seed), 6)
    return {
        "items": draw_items(jax.random.fold_in(key_list[5], 71), 0),
        "landmarks": draw_landmarks(jax.random.fold_in(key_list[5], 71), 0),
        "scales": jnp.clip(jnp.exp(math.log(1.0) - 1.3862944 * jax.random.uniform(key_list[2], (LANDMARKS,), jnp.float32) ** block_levels(key_list[2], (LANDMARKS,), ((0, 8),), -0.2, 0.2)), 0.25, 1.0),
        "eigvecs": normal_values(key_list[3], (LANDMARKS, K), LANDMARKS ** -0.5, 0.0625, ((0, 8),)),
        "eigvals": jnp.clip(jnp.exp(jax.random.uniform(key_list[4], (K,), jnp.float32, math.log(0.5), math.log(2.0))), 0.5, 2.0),
    }


def kernel_block(rows, landmarks, scales):
    row_vals = rows.astype(jnp.float32)
    land_vals = landmarks.astype(jnp.float32)
    row_sq = lax.optimization_barrier(jnp.sum(row_vals * row_vals, axis=1))
    land_sq = lax.optimization_barrier(jnp.sum(land_vals * land_vals, axis=1))
    cross = jnp.dot(rows, landmarks.T, preferred_element_type=jnp.float32)
    dist = row_sq[:, None] + land_sq[None, :] - 2.0 * cross
    return jnp.exp(-dist * scales[None, :])

def reference(items, landmarks, scales, eigvecs, eigvals):
    group = ROW_DEV * N_LAND
    blocks = items.reshape(NROWS // group, group, D)

    def first_pass(rows):
        kernel = kernel_block(rows, landmarks, scales)
        return (lax.optimization_barrier(jnp.sum(kernel, axis=0)), lax.optimization_barrier(jnp.sum(kernel, axis=1)))
    land_parts, row_degree = lax.map(first_pass, blocks)
    land_degree = lax.optimization_barrier(jnp.sum(land_parts, axis=0))
    factor = jnp.sqrt(jnp.float32(NROWS) * jnp.float32(LANDMARKS))

    def second_pass(inputs):
        rows, degrees = inputs
        kernel = kernel_block(rows, landmarks, scales)
        scaled = (kernel / jnp.sqrt(land_degree)[None, :]).astype(jnp.bfloat16)
        partial_value = jnp.dot(scaled, eigvecs, preferred_element_type=jnp.float32)
        coords = partial_value * (factor / jnp.sqrt(degrees))[:, None] / eigvals[None, :]
        outer = jnp.dot(coords.T, coords, precision=lax.Precision.HIGHEST)
        return (coords, outer)
    coords, outers = lax.map(second_pass, (blocks, row_degree))
    gram = lax.optimization_barrier(jnp.sum(outers, axis=0)) / jnp.float32(NROWS)
    return (coords.reshape(NROWS, K), gram)
```

```python
import functools
import math

import jax
import jax.numpy as jnp
from jax import lax
from jax.experimental import pallas as pl
from jax.experimental.pallas import tpu as pltpu
from jax.sharding import PartitionSpec as P

F32 = jnp.float32
B16 = jnp.bfloat16
EXTRA = 16
VMEM = pl.BlockSpec(memory_space=pltpu.VMEM)
SMEM = pl.BlockSpec(memory_space=pltpu.SMEM)
TRANS = (((1,), (1,)), ((), ()))


def split3(x):
    hi = x.astype(B16)
    rest = x - hi.astype(F32)
    mid = rest.astype(B16)
    return hi, mid, (rest - mid.astype(F32)).astype(B16)


def prep_body(pos_ref, land_ref, scale_ref, vec_ref, msg_ref, vmsg_ref):
    stripe, depth = land_ref.shape
    msg_ref[stripe:, :] = jnp.zeros((EXTRA, depth), B16)
    land = land_ref[...]
    msg_ref[:stripe, :] = land
    vmsg_ref[...] = vec_ref[...]
    vals = land.astype(F32)
    squares = vals * vals
    high = squares.astype(B16)
    low = (squares - high.astype(F32)).astype(B16)
    ones = jnp.ones((8, depth), B16)
    norm = lax.dot_general(ones, high, TRANS, preferred_element_type=F32)
    norm = norm + lax.dot_general(ones, low, TRANS, preferred_element_type=F32)
    rows = split3(scale_ref[0]) + split3(norm[:1])
    block = jnp.concatenate([r.astype(F32) for r in rows] + [jnp.zeros((EXTRA - 6, stripe), F32)], axis=0)
    msg_ref[stripe:, :stripe] = block.astype(B16)


def prep(pos, landmarks, scales, eigvecs, parts):
    count, depth = landmarks.shape
    stripe = count // parts
    width = eigvecs.shape[1]
    return pl.pallas_call(
        prep_body,
        grid_spec=pltpu.PrefetchScalarGridSpec(
            num_scalar_prefetch=1,
            grid=(1,),
            in_specs=[
                pl.BlockSpec((stripe, depth), lambda i, p: (p[0], 0)),
                pl.BlockSpec((1, 1, stripe), lambda i, p: (p[0], 0, 0)),
                pl.BlockSpec((stripe, width), lambda i, p: (p[0], 0)),
            ],
            out_specs=[
                pl.BlockSpec((stripe + EXTRA, depth), lambda i, p: (0, 0)),
                pl.BlockSpec((stripe, width), lambda i, p: (0, 0)),
            ],
        ),
        out_shape=[
            jax.ShapeDtypeStruct((stripe + EXTRA, depth), B16),
            jax.ShapeDtypeStruct((stripe, width), B16),
        ],
        name="prep",
    )(pos, landmarks, scales.reshape(parts, 1, stripe), eigvecs)


def block_body(*refs, groups, slot, chunk, first_col):
    nrow = sum(groups)
    rows = refs[:nrow]
    msgs = refs[nrow : nrow + 2]
    col_in = refs[nrow + 2]
    row_in = refs[nrow + 3 : nrow + 3 + len(groups)]
    outs = refs[nrow + 3 + len(groups) :]
    kern = outs[: len(groups)]
    col_out = outs[len(groups)]
    row_out = outs[len(groups) + 1 :]
    stripe = msgs[0].shape[0] - EXTRA
    log2e = math.log2(math.e)

    def triple(ref, at):
        part = ref[stripe:, :stripe].astype(F32)
        return part[at : at + 1] + part[at + 1 : at + 2] + part[at + 2 : at + 3]

    neg = [triple(m, 0) * (-log2e) for m in msgs]
    norm = [triple(m, 3) for m in msgs]
    cols = [jnp.zeros((8, stripe), F32) for _ in msgs]
    at = 0
    for g, pieces in enumerate(groups):
        base = 0
        for piece in range(pieces):
            src = rows[at]
            at += 1

            def step(i, carry, src=src, g=g, base=base):
                start = pl.multiple_of(i * chunk, chunk)
                block = src[pl.ds(start, chunk), :]
                vals = block.astype(F32)
                sq = jnp.sum(vals * vals, axis=1, keepdims=True)
                fresh = []
                lanes = jnp.zeros((chunk, 128), F32)
                for e, m in enumerate(msgs):
                    cross = lax.dot_general(block, m[:stripe, :], TRANS, preferred_element_type=F32)
                    dist = (sq + norm[e]) - 2.0 * cross
                    value = jnp.exp2(dist * neg[e])
                    kern[g][pl.ds(base + start, chunk), e * stripe : (e + 1) * stripe] = value
                    fresh.append(carry[e] + jnp.sum(value.reshape(chunk // 8, 8, stripe), axis=0))
                    for q in range(stripe // 128):
                        lanes = lanes + value[:, q * 128 : (q + 1) * 128]
                for q in range(chunk // 128):
                    row = jnp.sum(lanes[q * 128 : (q + 1) * 128].T, axis=0, keepdims=True)
                    spot = pl.ds(pl.multiple_of(base + start + q * 128, 128), 128)
                    row_out[g][:, spot] = row_in[g][:, spot] + row
                return tuple(fresh)

            cols = list(lax.fori_loop(0, src.shape[0] // chunk, step, tuple(cols)))
            base += src.shape[0]
    total = jnp.concatenate([jnp.sum(c, axis=0, keepdims=True) for c in cols], axis=1)
    if first_col:
        col_out[...] = total
    else:
        col_out[...] = col_in[...] + total


def block_call(row_groups, msgs, col_in, row_in, name):
    groups = tuple(len(g) for g in row_groups)
    flat = [r for g in row_groups for r in g]
    depth = flat[0].shape[1]
    stripe = msgs[0].shape[0] - EXTRA
    sizes = [sum(r.shape[0] for r in g) for g in row_groups]
    chunk = min(256, min(r.shape[0] for r in flat))
    out_shape = (
        [jax.ShapeDtypeStruct((n, 2 * stripe), F32) for n in sizes]
        + [jax.ShapeDtypeStruct((1, 2 * stripe), F32)]
        + [jax.ShapeDtypeStruct((1, n), F32) for n in sizes]
    )
    flops = 2 * sum(sizes) * 2 * stripe * depth
    outs = pl.pallas_call(
        functools.partial(block_body, groups=groups, slot=0, chunk=chunk, first_col=False),
        out_shape=out_shape,
        in_specs=[VMEM] * (len(flat) + 2 + 1 + len(groups)),
        out_specs=[VMEM] * len(out_shape),
        cost_estimate=pl.CostEstimate(flops=flops, bytes_accessed=0, transcendentals=sum(sizes) * 2 * stripe),
        compiler_params=pltpu.CompilerParams(vmem_limit_bytes=24 << 20),
        name=name,
    )(*flat, *msgs, col_in, *row_in)
    n = len(groups)
    return outs[:n], outs[n], outs[n + 1 :]


def apply_body(*refs, slots, peers):
    kern = refs[:slots]
    vecs = refs[slots : 3 * slots]
    degs = refs[3 * slots : 3 * slots + 1 + peers]
    out = refs[-1]
    stripe = vecs[0].shape[0]
    acc = None
    for k in range(slots):
        total = degs[0][k : k + 1, :]
        for j in range(1, peers + 1):
            total = total + degs[j][k ^ j : (k ^ j) + 1, :]
        weight = lax.rsqrt(total)
        for e in range(2):
            span = slice(e * stripe, (e + 1) * stripe)
            scaled = (kern[k][:, span] * weight[:, span]).astype(B16)
            term = jnp.dot(scaled, vecs[2 * k + e][...], preferred_element_type=F32)
            acc = term if acc is None else acc + term
    out[...] = acc.astype(out.dtype)


def apply_call(kern, vecs, degs, dtype, name):
    rows = kern[0].shape[0]
    width = vecs[0].shape[1]
    flops = 2 * rows * width * sum(v.shape[0] for v in vecs)
    return pl.pallas_call(
        functools.partial(apply_body, slots=len(kern), peers=len(degs) - 1),
        out_shape=jax.ShapeDtypeStruct((rows, width), dtype),
        in_specs=[VMEM] * (len(kern) + len(vecs) + len(degs)),
        out_specs=VMEM,
        cost_estimate=pl.CostEstimate(flops=flops, bytes_accessed=0, transcendentals=0),
        compiler_params=pltpu.CompilerParams(vmem_limit_bytes=24 << 20),
        name=name,
    )(*kern, *vecs, *degs)


def finish_body(core_ref, *refs, parts, factor):
    sums = refs[:parts]
    degs = refs[parts : 2 * parts]
    eig_ref = refs[2 * parts]
    coords_ref, keep_ref, send_ref = refs[2 * parts + 1 :]
    rows, width = coords_ref.shape
    half = width // 2
    deg = degs[0][...]
    for d in degs[1:]:
        deg = deg + d[...]
    gain = factor / jnp.sqrt(deg)
    inv = 1.0 / eig_ref[...]
    highs, lows = [], []
    for q in range(rows // 128):
        span = slice(q * 128, (q + 1) * 128)
        column = jnp.broadcast_to(gain[:, span], (128, 128)).T
        total = sums[0][span, :].astype(F32)
        for s in sums[1:]:
            total = total + s[span, :].astype(F32)
        value = jnp.concatenate(
            [total[:, k * 128 : (k + 1) * 128] * column for k in range(width // 128)], axis=1
        ) * inv
        coords_ref[span, :] = value
        high = value.astype(B16)
        highs.append(high)
        lows.append((value - high.astype(F32)).astype(B16))
    high = jnp.concatenate(highs, axis=0)
    low = jnp.concatenate(lows, axis=0)
    dims = (((0,), (0,)), ((), ()))
    outer = lax.dot_general(high, high, dims, preferred_element_type=F32)
    outer = outer + lax.dot_general(high, low, dims, preferred_element_type=F32)
    outer = outer + lax.dot_general(low, high, dims, preferred_element_type=F32)
    first = core_ref[0] == 0
    top, bottom = outer[:half], outer[half:]
    keep_ref[...] = jnp.where(first, top, bottom)
    send_ref[...] = jnp.where(first, bottom, top).astype(B16)


def finish_call(core, sums, degs, eigvals, factor):
    rows, width = sums[0].shape
    return pl.pallas_call(
        functools.partial(finish_body, parts=len(sums), factor=factor),
        out_shape=[
            jax.ShapeDtypeStruct((rows, width), F32),
            jax.ShapeDtypeStruct((width // 2, width), F32),
            jax.ShapeDtypeStruct((width // 2, width), B16),
        ],
        in_specs=[SMEM] + [VMEM] * (2 * len(sums) + 1),
        out_specs=[VMEM] * 3,
        compiler_params=pltpu.CompilerParams(vmem_limit_bytes=24 << 20),
        name="finish",
    )(core, *sums, *degs, eigvals.reshape(1, width))


def exchange(x, axis, offset):
    size = lax.axis_size(axis)
    return lax.ppermute(x, axis, [(i, i ^ offset) for i in range(size)])


def gather_rows(x, size):
    if size != 4:
        return [[x]] + [[exchange(x, "dp", d)] for d in range(1, size)]
    half = x.shape[0] // 2
    one = exchange(x, "dp", 1)
    two = exchange(x, "dp", 2)
    return [[x], [one], [two], [exchange(one[:half], "dp", 2), exchange(two[half:], "dp", 1)]]


def gather_chips(x, chips):
    if chips != 4:
        return [x] + [exchange(x, "land", 2 * k) for k in range(1, chips)]
    two = exchange(x, "land", 4)
    one = exchange(x, "land", 2)
    inner = lax.ppermute(x, "land", [(2, 4), (3, 5), (4, 2), (5, 3)])
    outer = lax.ppermute(two, "land", [(4, 6), (5, 7), (2, 0), (3, 1)])
    edge = lax.axis_index("land") // 2
    three = jnp.where((edge == 0) | (edge == chips - 1), outer, inner)
    return [x, one, two, three]


def per_device(items, landmarks, scales, eigvecs, eigvals):
    dp = lax.axis_size("dp")
    land = lax.axis_size("land")
    chips = land // 2
    own = items.shape[0]
    width = eigvecs.shape[1]
    rows_all = own * dp * land
    landmark_count = landmarks.shape[0] * land
    pos = lax.axis_index("dp").astype(jnp.int32).reshape(1)
    core = (lax.axis_index("land") % 2).astype(jnp.int32).reshape(1)

    msg, vmsg = prep(pos, landmarks, scales, eigvecs, dp)
    stripe = vmsg.shape[0]
    row_sets = gather_rows(items, dp)
    mine = gather_chips(msg, chips)
    mates = [exchange(m, "land", 1) for m in mine]
    vmsg, _ = lax.optimization_barrier((vmsg, mine[-1]))
    vmine = gather_chips(vmsg, chips)
    vmates = [exchange(m, "land", 1) for m in vmine]

    kern = [[None] * chips for _ in range(dp)]
    col = [jnp.zeros((1, 2 * stripe), F32) for _ in range(chips)]
    row = [jnp.zeros((1, own), F32) for _ in range(dp)]
    plan = [[0]] + ([[1, 2], [3]] if dp == 4 else [[d] for d in range(1, dp)])
    for group in plan:
        for k in range(chips):
            sets = [row_sets[d] for d in group]
            out, col[k], rows_out = block_call(sets, (mine[k], mates[k]), col[k], [row[d] for d in group], f"block{group[0]}_{k}")
            for i, d in enumerate(group):
                kern[d][k] = out[i]
                row[d] = rows_out[i]

    deg = jnp.concatenate(col, axis=0)
    mate = exchange(deg, "land", 1)
    deg = deg + jnp.concatenate([mate[:, stripe:], mate[:, :stripe]], axis=1)
    degs = [deg] + [exchange(deg, "land", 2 * k) for k in range(1, chips)]
    row_deg = [row[0]] + [exchange(row[d], "dp", d) for d in range(1, dp)]
    vecs = [v for pair in zip(vmine, vmates) for v in pair]

    sums = [None] * dp
    for d in list(range(dp - 1, 0, -1)) + [0]:
        part = apply_call(kern[d], vecs, degs, B16 if d else F32, f"apply{d}")
        sums[d] = exchange(part, "dp", d) if d else part

    factor = math.sqrt(float(rows_all) * float(landmark_count))
    coords, keep, send = finish_call(core, sums, row_deg, eigvals, factor)
    total = keep + exchange(send, "land", 1).astype(F32)
    for axis, size in (("dp", dp), ("land", land)):
        step = 1 if axis == "dp" else 2
        while step < size:
            total = lax.reduce_precision(total, 8, 7)
            total = total + exchange(total.astype(B16), axis, step).astype(F32)
            step *= 2
    total = total * (1.0 / rows_all)
    other = exchange(total, "land", 1)
    first = (core == 0).reshape(1, 1)
    gram = jnp.concatenate([jnp.where(first, total, other), jnp.where(first, other, total)], axis=0)
    return (coords, gram)


def solution(mesh):
    return jax.shard_map(
        per_device,
        mesh=mesh,
        in_specs=(P(("dp", "land"), None), P("land", None), P("land"), P("land", None), P()),
        out_specs=(P(("dp", "land"), None), P()),
        check_vma=False,
    )
```

```python
import functools
import math

import jax
import jax.numpy as jnp
from jax import lax
from jax.experimental import pallas as pl
from jax.experimental.pallas import tpu as pltpu
from jax.sharding import PartitionSpec as P

F32 = jnp.float32
B16 = jnp.bfloat16
EXTRA = 16
VMEM = pl.BlockSpec(memory_space=pltpu.VMEM)
SMEM = pl.BlockSpec(memory_space=pltpu.SMEM)
LIMIT = 8 << 20
TRANS = (((1,), (1,)), ((), ()))


def split3(x):
    hi = x.astype(B16)
    rest = x - hi.astype(F32)
    mid = rest.astype(B16)
    return hi, mid, (rest - mid.astype(F32)).astype(B16)


def prep_body(pos_ref, land_ref, scale_ref, vec_ref, msg_ref, vmsg_ref):
    stripe, depth = land_ref.shape
    msg_ref[stripe:, :] = jnp.zeros((EXTRA, depth), B16)
    land = land_ref[...]
    msg_ref[:stripe, :] = land
    vmsg_ref[...] = vec_ref[...]
    vals = land.astype(F32)
    squares = vals * vals
    high = squares.astype(B16)
    low = (squares - high.astype(F32)).astype(B16)
    ones = jnp.ones((8, depth), B16)
    norm = lax.dot_general(ones, high, TRANS, preferred_element_type=F32)
    norm = norm + lax.dot_general(ones, low, TRANS, preferred_element_type=F32)
    rows = split3(scale_ref[0]) + split3(norm[:1])
    block = jnp.concatenate([r.astype(F32) for r in rows] + [jnp.zeros((EXTRA - 6, stripe), F32)], axis=0)
    msg_ref[stripe:, :stripe] = block.astype(B16)


def in_hbm(x):
    return pltpu.with_memory_space_constraint(x, pltpu.HBM)


def prep(pos, landmarks, scales, eigvecs, parts):
    count, depth = landmarks.shape
    stripe = count // parts
    width = eigvecs.shape[1]
    return pl.pallas_call(
        prep_body,
        grid_spec=pltpu.PrefetchScalarGridSpec(
            num_scalar_prefetch=1,
            grid=(1,),
            in_specs=[
                pl.BlockSpec((stripe, depth), lambda i, p: (p[0], 0)),
                pl.BlockSpec((1, 1, stripe), lambda i, p: (p[0], 0, 0)),
                pl.BlockSpec((stripe, width), lambda i, p: (p[0], 0)),
            ],
            out_specs=[
                pl.BlockSpec((stripe + EXTRA, depth), lambda i, p: (0, 0)),
                pl.BlockSpec((stripe, width), lambda i, p: (0, 0)),
            ],
        ),
        out_shape=[
            jax.ShapeDtypeStruct((stripe + EXTRA, depth), B16),
            jax.ShapeDtypeStruct((stripe, width), B16),
        ],
        compiler_params=pltpu.CompilerParams(vmem_limit_bytes=LIMIT),
        name="prep",
    )(pos, in_hbm(landmarks), scales.reshape(parts, 1, stripe), in_hbm(eigvecs))


def block_body(*refs, groups):
    nrow = sum(groups)
    rows = refs[:nrow]
    msgs = refs[nrow : nrow + 2]
    col_in = refs[nrow + 2]
    row_in = refs[nrow + 3 : nrow + 3 + len(groups)]
    outs = refs[nrow + 3 + len(groups) :]
    kern = outs[: len(groups)]
    col_out = outs[len(groups)]
    row_out = outs[len(groups) + 1 :]
    stripe = msgs[0].shape[0] - EXTRA
    log2e = math.log2(math.e)

    def triple(ref, at):
        part = ref[stripe:, :stripe].astype(F32)
        return part[at : at + 1] + part[at + 1 : at + 2] + part[at + 2 : at + 3]

    neg = [triple(m, 0) * (-log2e) for m in msgs]
    norm = [triple(m, 3) for m in msgs]
    cols = [jnp.zeros((8, stripe), F32) for _ in msgs]
    at = 0
    for g, pieces in enumerate(groups):
        base = 0
        for _ in range(pieces):
            src = rows[at]
            at += 1

            size = src.shape[0]
            block = src[...]
            vals = block.astype(F32)
            sq = jnp.sum(vals * vals, axis=1, keepdims=True)
            lanes = jnp.zeros((size, 128), F32)
            for e, m in enumerate(msgs):
                cross = lax.dot_general(block, m[:stripe, :], TRANS, preferred_element_type=F32)
                dist = (sq + norm[e]) - 2.0 * cross
                value = jnp.exp2(dist * neg[e])
                kern[g][base : base + size, e * stripe : (e + 1) * stripe] = value
                cols[e] = cols[e] + jnp.sum(value.reshape(size // 8, 8, stripe), axis=0)
                for q in range(stripe // 128):
                    lanes = lanes + value[:, q * 128 : (q + 1) * 128]
            for q in range(size // 128):
                row = jnp.sum(lanes[q * 128 : (q + 1) * 128].T, axis=0, keepdims=True)
                spot = slice(base + q * 128, base + (q + 1) * 128)
                row_out[g][:, spot] = row_in[g][:, spot] + row
            base += size
    total = jnp.concatenate([jnp.sum(c, axis=0, keepdims=True) for c in cols], axis=1)
    col_out[...] = col_in[...] + total


def block_call(row_groups, msgs, col_in, row_in):
    groups = tuple(len(g) for g in row_groups)
    flat = [r for g in row_groups for r in g]
    depth = flat[0].shape[1]
    stripe = msgs[0].shape[0] - EXTRA
    sizes = [sum(r.shape[0] for r in g) for g in row_groups]
    out_shape = (
        [jax.ShapeDtypeStruct((n, 2 * stripe), F32) for n in sizes]
        + [jax.ShapeDtypeStruct((1, 2 * stripe), F32)]
        + [jax.ShapeDtypeStruct((1, n), F32) for n in sizes]
    )
    flops = 2 * sum(sizes) * 2 * stripe * depth
    outs = pl.pallas_call(
        functools.partial(block_body, groups=groups),
        out_shape=out_shape,
        in_specs=[VMEM] * (len(flat) + 2 + 1 + len(groups)),
        out_specs=[VMEM] * len(out_shape),
        cost_estimate=pl.CostEstimate(flops=flops, bytes_accessed=0, transcendentals=sum(sizes) * 2 * stripe),
        compiler_params=pltpu.CompilerParams(vmem_limit_bytes=LIMIT),
    )(*flat, *msgs, col_in, *row_in)
    n = len(groups)
    return outs[:n], outs[n], outs[n + 1 :]


def apply_body(*refs, slots, peers, tail):
    kern = refs[:slots]
    vecs = refs[slots : 3 * slots]
    degs = refs[3 * slots : 3 * slots + 1 + peers]
    out = refs[-1]
    stripe, width = vecs[0].shape
    rows = kern[0].shape[0]
    acc = None
    for k in range(slots):
        total = degs[0][k : k + 1, :]
        for j in range(1, peers + 1):
            total = total + degs[j][k ^ j : (k ^ j) + 1, :]
        weight = lax.rsqrt(total)
        for e in range(2):
            span = slice(e * stripe, (e + 1) * stripe)
            scaled = (kern[k][:, span] * weight[:, span]).astype(B16)
            term = jnp.dot(scaled, vecs[2 * k + e][...], preferred_element_type=F32)
            acc = term if acc is None else acc + term
    out[:rows, :] = acc.astype(out.dtype)
    if tail:
        sums = refs[-2]
        parts = []
        for at in range(0, rows, width):
            parts += [p.astype(F32) for p in split3(sums[:, at : at + width])]
        parts.append(jnp.zeros((EXTRA - len(parts), width), F32))
        out[rows:, :] = jnp.concatenate(parts, axis=0).astype(B16)


def apply_call(kern, vecs, degs, row_sum):
    rows = kern[0].shape[0]
    width = vecs[0].shape[1]
    tail = row_sum is not None
    operands = [*kern, *vecs, *degs] + ([row_sum] if tail else [])
    flops = 2 * rows * width * sum(v.shape[0] for v in vecs)
    return pl.pallas_call(
        functools.partial(apply_body, slots=len(kern), peers=len(degs) - 1, tail=tail),
        out_shape=jax.ShapeDtypeStruct((rows + EXTRA * tail, width), B16 if tail else F32),
        in_specs=[VMEM] * len(operands),
        out_specs=VMEM,
        cost_estimate=pl.CostEstimate(flops=flops, bytes_accessed=0, transcendentals=0),
        compiler_params=pltpu.CompilerParams(vmem_limit_bytes=LIMIT),
    )(*operands)


def finish_body(core_ref, *refs, parts, factor):
    sums = refs[:parts]
    deg_ref, eig_ref, coords_ref, keep_ref, send_ref = refs[parts:]
    rows, width = coords_ref.shape
    half = width // 2
    deg = deg_ref[...]
    for s in sums[1:]:
        tail = s[rows:, :].astype(F32)
        pieces = [tail[3 * i : 3 * i + 1] + tail[3 * i + 1 : 3 * i + 2] + tail[3 * i + 2 : 3 * i + 3] for i in range(rows // width)]
        deg = deg + jnp.concatenate(pieces, axis=1)
    gain = factor / jnp.sqrt(deg)
    inv = 1.0 / eig_ref[...]
    highs, lows = [], []
    for q in range(rows // 128):
        span = slice(q * 128, (q + 1) * 128)
        column = jnp.broadcast_to(gain[:, span], (128, 128)).T
        total = sums[0][span, :].astype(F32)
        for s in sums[1:]:
            total = total + s[span, :].astype(F32)
        value = jnp.concatenate(
            [total[:, k * 128 : (k + 1) * 128] * column for k in range(width // 128)], axis=1
        ) * inv
        coords_ref[span, :] = value
        high = value.astype(B16)
        highs.append(high)
        lows.append((value - high.astype(F32)).astype(B16))
    high = jnp.concatenate(highs, axis=0)
    low = jnp.concatenate(lows, axis=0)
    dims = (((0,), (0,)), ((), ()))
    outer = lax.dot_general(high, high, dims, preferred_element_type=F32)
    outer = outer + lax.dot_general(high, low, dims, preferred_element_type=F32)
    outer = outer + lax.dot_general(low, high, dims, preferred_element_type=F32)
    first = core_ref[1] == 0
    top, bottom = outer[:half], outer[half:]
    keep_ref[...] = jnp.where(first, top, bottom)
    send_ref[...] = jnp.where(first, bottom, top).astype(B16)


def finish_call(core, sums, deg, eigvals, factor):
    rows, width = sums[0].shape
    return pl.pallas_call(
        functools.partial(finish_body, parts=len(sums), factor=factor),
        out_shape=[
            jax.ShapeDtypeStruct((rows, width), F32),
            jax.ShapeDtypeStruct((width // 2, width), F32),
            jax.ShapeDtypeStruct((width // 2, width), B16),
        ],
        in_specs=[SMEM] + [VMEM] * (len(sums) + 2),
        out_specs=[VMEM] * 3,
        compiler_params=pltpu.CompilerParams(vmem_limit_bytes=LIMIT),
        name="finish",
    )(core, *sums, deg, eigvals.reshape(1, width))


def join_body(core_ref, own_ref, other_ref, out_ref, *, scale):
    half = own_ref.shape[0]
    first = core_ref[1] == 0
    own, other = own_ref[...] * scale, other_ref[...] * scale
    out_ref[:half] = jnp.where(first, own, other)
    out_ref[half:] = jnp.where(first, other, own)


def join_call(core, own, other, scale):
    half, width = own.shape
    return pl.pallas_call(
        functools.partial(join_body, scale=scale),
        out_shape=jax.ShapeDtypeStruct((2 * half, width), F32),
        in_specs=[SMEM, VMEM, VMEM],
        out_specs=VMEM,
        compiler_params=pltpu.CompilerParams(vmem_limit_bytes=LIMIT),
        name="join",
    )(core, own, other)


def exchange(x, axis, offset):
    size = lax.axis_size(axis)
    return lax.ppermute(x, axis, [(i, i ^ offset) for i in range(size)])


def after(x, *others):
    return lax.optimization_barrier((x, *others))[0]


def per_device(items, landmarks, scales, eigvecs, eigvals):
    dp = lax.axis_size("dp")
    land = lax.axis_size("land")
    chips = land // 2
    own = items.shape[0]
    rows_all = own * dp * land
    landmark_count = landmarks.shape[0] * land
    pos = jnp.stack([lax.axis_index("dp"), lax.axis_index("land") & 1]).astype(jnp.int32)
    small = dp == 4 and chips == 4

    kern = [[None] * chips for _ in range(dp)]
    row = [jnp.zeros((1, own), F32) for _ in range(dp)]
    token = [None]

    def block(group, k, mine, mates, col):
        if token[0] is not None:
            col[k] = after(col[k], token[0])
        out, col[k], rows_out = block_call(
            [row_sets[d] for d in group], (mine[k], mates[k]), col[k], [row[d] for d in group]
        )
        for i, d in enumerate(group):
            kern[d][k] = out[i]
            row[d] = rows_out[i]
        token[0] = col[k]

    def line_gather(x, ready=None):
        if chips != 4:
            return [x] + [exchange(x, "land", 2 * k) for k in range(1, chips)]
        two = exchange(x, "land", 4)
        one = exchange(x, "land", 2)
        inner = lax.ppermute(x, "land", [(2, 4), (3, 5), (4, 2), (5, 3)])
        relay = two if ready is None else after(two, *ready())
        outer = lax.ppermute(relay, "land", [(4, 6), (5, 7), (2, 0), (3, 1)])
        return [x, one, two, inner + outer]

    mates = [None] * chips
    if small:
        half = own // 2
        upper, lower = items[:half], items[half:]
        row_sets = [[items], [exchange(upper, "dp", 1)], [exchange(lower, "dp", 2)]]
        msg, vmsg = prep(pos, landmarks, scales, eigvecs, dp)
        stripe = vmsg.shape[0]
        col = [jnp.zeros((1, 2 * stripe), F32) for _ in range(chips)]
        mates[0] = exchange(msg, "land", 1)
        mine = [msg]
        row_sets[1].append(exchange(lower, "dp", 1))
        row_sets[2].insert(0, exchange(upper, "dp", 2))
        row_sets.append([exchange(row_sets[1][0], "dp", 2), exchange(row_sets[2][1], "dp", 1)])
        block([0], 0, mine, mates, col)
        block([1, 2], 0, mine, mates, col)
        seen = token[0]
        mine = line_gather(msg, lambda: (seen,))
        for k in (2, 1):
            mates[k] = exchange(mine[k], "land", 1)
            block([0], k, mine, mates, col)
            block([1, 2], k, mine, mates, col)
        vmine = line_gather(after(vmsg, token[0]))
        for k in (0, 2, 1):
            block([3], k, mine, mates, col)
        mates[3] = exchange(mine[3], "land", 1)
        for group in ([0], [1, 2], [3]):
            block(group, 3, mine, mates, col)
    else:
        row_sets = [[items]] + [[exchange(items, "dp", d)] for d in range(1, dp)]
        msg, vmsg = prep(pos, landmarks, scales, eigvecs, dp)
        stripe = vmsg.shape[0]
        col = [jnp.zeros((1, 2 * stripe), F32) for _ in range(chips)]
        mine = line_gather(msg)
        mates = [exchange(m, "land", 1) for m in mine]
        vmine = line_gather(vmsg)
        for d in range(dp):
            for k in range(chips):
                block([d], k, mine, mates, col)
    vmates = [exchange(m, "land", 1) for m in vmine]

    deg = jnp.concatenate(col, axis=0)
    mate = exchange(deg, "land", 1)
    deg = deg + jnp.concatenate([mate[:, stripe:], mate[:, :stripe]], axis=1)
    degs = [deg] + [exchange(deg, "land", 2 * k) for k in range(chips - 1, 0, -1)][::-1]
    vecs = [v for pair in zip(vmine, vmates) for v in pair]

    sums = [None] * dp
    last = None
    for d in list(range(dp - 1, 0, -1)) + [0]:
        if last is not None:
            degs = [after(degs[0], last)] + degs[1:]
        part = apply_call(kern[d], vecs, degs, row[d] if d else None)
        last = part
        sums[d] = exchange(part, "dp", d) if d else part

    factor = math.sqrt(float(rows_all) * float(landmark_count))
    coords, keep, send = finish_call(pos, sums, row[0], eigvals, factor)
    total = keep + exchange(send, "land", 1).astype(F32)
    for axis, size in (("dp", dp), ("land", land)):
        step = 1 if axis == "dp" else 2
        while step < size:
            total = lax.reduce_precision(total, 8, 7)
            total = total + exchange(total.astype(B16), axis, step).astype(F32)
            step *= 2
    other = exchange(total, "land", 1)
    gram = join_call(pos, total, other, 1.0 / rows_all)
    return (coords, gram)


def solution(mesh):
    return jax.shard_map(
        per_device,
        mesh=mesh,
        in_specs=(P(("dp", "land"), None), P("land", None), P("land"), P("land", None), P()),
        out_specs=(P(("dp", "land"), None), P()),
        check_vma=False,
    )
```
